32 devices in a mesh: dp: 1 (over z), tp: 32 (over x, y, core).
Axes of the slice: x: 4, y: 4, z: 1, core: 2. Of those that a mesh axis runs over, the one named last changes fastest.
The devices are a block of a 4x4x8 slice.
Arguments:
- x: bfloat16 [4096, 8192], P(('dp', 'tp'))
- dy: bfloat16 [4096, 8192], P(('dp', 'tp'))
- gate: bfloat16 [4096, 24576], P('dp', 'tp')
- up: bfloat16 [4096, 24576], P('dp', 'tp')
- w_gate: bfloat16 [8192, 24576], P(None, 'tp')
- w_up: bfloat16 [8192, 24576], P(None, 'tp')
- w_down: bfloat16 [24576, 8192], P('tp')
Outputs:
- output 1: bfloat16 [4096, 8192], P(('dp', 'tp'))
- output 2: bfloat16 [8192, 24576], P('dp', 'tp')
- output 3: bfloat16 [8192, 24576], P('dp', 'tp')
- output 4: bfloat16 [24576, 8192], P(('dp', 'tp'))
All inputs are finite; a program needn't handle non-finite values.
Results may differ from the reference program's by a relative error of at most 0.012.
Values are sent between devices in bfloat16 or wider.
A program may use at most 768 MiB of HBM per device.

```python
import jax
import jax.numpy as jnp

ROWS = 4096
D = 8192
FF = 24576


def act(gate, up):
    return jax.nn.silu(gate) * up


def setup_inputs(seed: int = 0, part: int = 0) -> dict:
    kx, ky, ka, kb, kg, ku, kd = jax.random.split(jax.random.key(seed), 7)
    kx, ky, ka, kb = (jax.random.fold_in(k, part) for k in (kx, ky, ka, kb))
    drawn = {
        "x": jax.random.normal(kx, (ROWS, D), jnp.float32),
        "dy": jax.random.normal(ky, (ROWS, D), jnp.float32),
        "gate": jax.random.normal(ka, (ROWS, FF), jnp.float32),
        "up": jax.random.normal(kb, (ROWS, FF), jnp.float32),
        "w_gate": jax.random.normal(kg, (D, FF), jnp.float32) * D**-0.5,
        "w_up": jax.random.normal(ku, (D, FF), jnp.float32) * D**-0.5,
        "w_down": jax.random.normal(kd, (FF, D), jnp.float32) * FF**-0.5,
    }
    return {k: v.astype(jnp.bfloat16) for k, v in drawn.items()}


def reference(x, dy, gate, up, w_gate, w_up, w_down):
    hidden, back = jax.vjp(act, gate.astype(jnp.float32), up.astype(jnp.float32))
    d_hidden = jnp.dot(dy, w_down.T, preferred_element_type=jnp.float32)
    d_gate, d_up = (g.astype(jnp.bfloat16) for g in back(d_hidden))
    dx = jnp.dot(d_gate, w_gate.T, preferred_element_type=jnp.float32) + jnp.dot(d_up, w_up.T, preferred_element_type=jnp.float32)
    dw_gate = jnp.dot(x.T, d_gate, preferred_element_type=jnp.float32)
    dw_up = jnp.dot(x.T, d_up, preferred_element_type=jnp.float32)
    dw_down = jnp.dot(hidden.astype(jnp.bfloat16).T, dy, preferred_element_type=jnp.float32)
    return tuple(g.astype(jnp.bfloat16) for g in (dx, dw_gate, dw_up, dw_down))
```

```python
import functools
import math

import jax
import jax.numpy as jnp
from jax import lax
from jax.experimental import pallas as pl
from jax.experimental.pallas import tpu as pltpu
from jax.sharding import PartitionSpec as P

F32, BF16 = jnp.float32, jnp.bfloat16
RINGS = 4
HALVES = 2


def act(gate, up):
    return jax.nn.silu(gate) * up


def place(k):
    me = lax.axis_index("tp")
    core, chip = me % 2, me // 2
    a, b = chip // k, chip % k
    s = (a + b) % k
    return core, a, b, (a * k + s, b * k + s)


def chip_at(k, cycle, position):
    a = position // k
    b = (position % k - a + k) % k
    return a * k + b if cycle == 0 else b * k + a


def on_ring(ring, position, steps, chips):
    return (position + steps + chips) % chips if ring % 2 == 0 else (position - steps + chips) % chips


def greet(k, core, a, b):
    chips = (((a + 1) % k) * k + b, ((a + k - 1) % k) * k + b, a * k + (b + 1) % k, a * k + (b + k - 1) % k)
    barrier = pltpu.get_barrier_semaphore()
    for chip in chips:
        pl.semaphore_signal(barrier, inc=1, device_id={"tp": chip * 2 + core})
    pl.semaphore_signal(barrier, inc=1, device_id={"tp": (a * k + b) * 2 + 1 - core})
    pl.semaphore_wait(barrier, 5)


def scatter_kernel(k, dg, du, wg, wu, out, wv, av, own, psend, precv, rsend, rrecv,
                   w_sem, a_sem, psend_sem, precv_sem, rsend_sem, rrecv_sem, out_sem):
    chips = k * k
    units, width, depth = wv.shape
    rows, ff = out.shape[0], depth // 2
    core, a, b, positions = place(k)
    partner = (a * k + b) * 2 + 1 - core
    order = [(r * HALVES + h, r, h) for h in range(HALVES) for r in range(RINGS)]

    def w_copies(u):
        cols = pl.ds(u * width, width)
        return [pltpu.make_async_copy(w.at[cols], wv.at[u, :, pl.ds(i * ff, ff)], w_sem.at[u, i]) for i, w in enumerate((wg, wu))]

    def a_copies(s, r):
        to = chip_at(k, r // 2, on_ring(r, positions[r // 2], -1 - s + chips, chips))
        copies = []
        for i, which in enumerate((core, 1 - core)):
            at = pl.ds((to * 2 + which) * rows, rows)
            for j, d in enumerate((dg, du)):
                copies.append(pltpu.make_async_copy(
                    d.at[at], av.at[s % 2, r, pl.ds(i * rows, rows), pl.ds(j * ff, ff)], a_sem.at[s % 2, r, 2 * i + j]))
        return copies

    def to_partner(s, u):
        return pltpu.make_async_remote_copy(
            psend.at[u], precv.at[s % 2, u], psend_sem.at[u], precv_sem.at[s % 2, u], device_id={"tp": partner})

    def to_next(s, u, r):
        to = chip_at(k, r // 2, on_ring(r, positions[r // 2], 1, chips)) * 2 + core
        return pltpu.make_async_remote_copy(
            rsend.at[s % 2, u], rrecv.at[(s + 1) % 3, u], rsend_sem.at[s % 2, u], rrecv_sem.at[(s + 1) % 3, u], device_id={"tp": to})

    def to_out(u):
        return pltpu.make_async_copy(rsend.at[(chips - 1) % 2, u], out.at[:, pl.ds(u * width, width)], out_sem.at[u])

    def multiply(s, u, r, h, first=False):
        if first:
            for c in w_copies(u):
                c.wait()
        if h == 0:
            for c in a_copies(s, r):
                c.wait()
        if not first:
            to_partner(s, u).wait_send()
        acc = lax.dot_general(av[s % 2, r], wv[u], (((1,), (1,)), ((), ())), preferred_element_type=F32)
        own[u] = acc[:rows]
        psend[u] = acc[rows:].astype(BF16)
        to_partner(s, u).start()

    def combine(s, u, r):
        to_partner(s, u).wait_recv()

        @pl.when(s >= 2)
        def _():
            to_next(s, u, r).wait_send()

        @pl.when(s == 0)
        def _():
            rsend[s % 2, u] = (own[u] + precv[s % 2, u].astype(F32)).astype(BF16)

        @pl.when(s > 0)
        def _():
            to_next(s - 1, u, r).wait_recv()
            rsend[s % 2, u] = (own[u] + precv[s % 2, u].astype(F32) + rrecv[s % 3, u].astype(F32)).astype(BF16)

        @pl.when(s < chips - 1)
        def _():
            to_next(s, u, r).start()

        @pl.when(s == chips - 1)
        def _():
            to_out(u).start()

    for u, r, h in order:
        if h == 0:
            for c in a_copies(0, r):
                c.start()
        for c in w_copies(u):
            c.start()
    for r in range(RINGS):
        for c in a_copies(1, r):
            c.start()
    greet(k, core, a, b)
    for u, r, h in order:
        multiply(0, u, r, h, first=True)

    @pl.loop(0, chips)
    def _(s):
        @pl.when(s + 2 < chips)
        def _():
            for r in range(RINGS):
                for c in a_copies(s + 2, r):
                    c.start()
        for u, r, h in order:
            combine(s, u, r)

            @pl.when(s + 1 < chips)
            def _():
                multiply(s + 1, u, r, h)

    for u, r, h in order:
        to_partner(chips - 1, u).wait_send()
        to_next(chips - 2, u, r).wait_send()
        to_out(u).wait()


def scatter_dx(k, dg, du, wg, wu):
    tokens, ff = dg.shape
    d = wg.shape[0]
    rows = tokens // (2 * k * k)
    units = RINGS * HALVES
    width = d // units
    dma = pltpu.SemaphoreType.DMA
    return pl.pallas_call(
        functools.partial(scatter_kernel, k),
        out_shape=jax.ShapeDtypeStruct((rows, d), BF16),
        in_specs=[pl.BlockSpec(memory_space=pl.ANY)] * 4,
        out_specs=pl.BlockSpec(memory_space=pl.ANY),
        scratch_shapes=[
            pltpu.VMEM((units, width, 2 * ff), BF16),
            pltpu.VMEM((2, RINGS, 2 * rows, 2 * ff), BF16),
            pltpu.VMEM((units, rows, width), F32),
            pltpu.VMEM((units, rows, width), BF16),
            pltpu.VMEM((2, units, rows, width), BF16),
            pltpu.VMEM((2, units, rows, width), BF16),
            pltpu.VMEM((3, units, rows, width), BF16),
            dma((units, 2)), dma((2, RINGS, 4)), dma((units,)), dma((2, units)), dma((2, units)), dma((3, units)), dma((units,)),
        ],
        compiler_params=pltpu.CompilerParams(collective_id=0, has_side_effects=True, vmem_limit_bytes=63 * 2**20),
        cost_estimate=pl.CostEstimate(flops=4 * tokens * ff * d, bytes_accessed=6 * tokens * ff + 4 * d * ff, transcendentals=0),
        name="scatter_dx",
    )(dg, du, wg, wu)


SLOTS = 4


def gather(k, passes, core, a, b, positions, src, slots, load_sem, next_sem, ring_sem, mate_send_sem, mate_sem, credit, before, pieces, after):
    chips = k * k
    total = passes * chips
    share, cols = slots.shape[1] // (2 * RINGS), slots.shape[2]
    width = cols // HALVES
    partner = (a * k + b) * 2 + 1 - core

    def part(g, r, h, which=core):
        at = pl.multiple_of((2 * r + which) * share, share)
        return slots.at[g % SLOTS, pl.ds(at, share), pl.ds(h * width, width)]

    def load(g, r, h):
        at = pl.multiple_of(g // chips * cols + h * width, width)
        return pltpu.make_async_copy(src.at[pl.ds(r * share, share), pl.ds(at, width)], part(g, r, h), load_sem.at[r, h])

    def to_next(g, r, h):
        to = chip_at(k, r // 2, on_ring(r, positions[r // 2], 1, chips)) * 2 + core
        return pltpu.make_async_remote_copy(
            part(g, r, h), part(g + 1, r, h), next_sem.at[g % 2, r, h], ring_sem.at[(g + 1) % SLOTS, r, h], device_id={"tp": to})

    def to_mate(g, r, h):
        return pltpu.make_async_remote_copy(
            part(g, r, h), part(g, r, h), mate_send_sem.at[g % 2, r, h], mate_sem.at[g % SLOTS, r, h], device_id={"tp": partner})

    def came_from_mate(g, r, h):
        return pltpu.make_async_remote_copy(
            part(g, r, h), part(g, r, h, 1 - core), mate_send_sem.at[g % 2, r, h], mate_sem.at[g % SLOTS, r, h], device_id={"tp": partner})

    def pass_on(g, r, h):
        @pl.when(g % chips == 0)
        def _():
            load(g, r, h).wait()

        @pl.when(g % chips > 0)
        def _():
            to_next(g - 1, r, h).wait_recv()

        @pl.when(g % chips < chips - 1)
        def _():
            if h == 0:
                @pl.when(g + 1 >= SLOTS)
                def _():
                    pl.semaphore_wait(credit.at[r], 1)
            to_next(g, r, h).start()
        to_mate(g, r, h).start()

    both = [(r, h) for h in range(HALVES) for r in range(RINGS)]
    for r, h in both:
        load(0, r, h).start()
    greet(k, core, a, b)

    @pl.loop(0, total + 1)
    def _(g):
        for h in range(HALVES):
            @pl.when(g < total)
            def _():
                for r in range(RINGS):
                    pass_on(g, r, h)

            @pl.when(g > 0)
            def _():
                if h == 0:
                    for r, half in both:
                        came_from_mate(g - 1, r, half).wait_recv()
                    before(g - 1)
                pieces[h](g - 1)

        @pl.when(g > 0)
        def _():
            after(g - 1)
            for r, h in both:
                @pl.when((g - 1) % chips < chips - 1)
                def _():
                    to_next(g - 1, r, h).wait_send()
                to_mate(g - 1, r, h).wait_send()
            refill = g - 1 + SLOTS

            @pl.when(jnp.logical_and(refill < total, refill % chips > 0))
            def _():
                for r in range(RINGS):
                    frm = chip_at(k, r // 2, on_ring(r, positions[r // 2], -1, chips)) * 2 + core
                    pl.semaphore_signal(credit.at[r], inc=1, device_id={"tp": frm})

            @pl.when(jnp.logical_and(refill < total, refill % chips == 0))
            def _():
                for r, h in both:
                    load(refill, r, h).start()


def gather_scratch(rows, cols):
    dma, two = pltpu.SemaphoreType.DMA, (2, RINGS, HALVES)
    return [
        pltpu.VMEM((SLOTS, 2 * rows, cols), BF16),
        dma((RINGS, HALVES)), dma(two), dma((SLOTS, RINGS, HALVES)), dma(two), dma((SLOTS, RINGS, HALVES)),
        pltpu.SemaphoreType.REGULAR((RINGS,)),
    ]


def token_rows(k, positions, g, share, rows):
    chips = k * k
    for r in range(RINGS):
        chip = chip_at(k, r // 2, on_ring(r, positions[r // 2], -(g % chips), chips))
        for c in range(2):
            yield (2 * r + c) * share, pl.multiple_of((chip * 2 + c) * rows + r * share, share)


def hidden_kernel(k, dy, gate, up, w_down, dg, du, dw, wd, wacc, hacc, given, hid, grads, *rest):
    (w_sem, given_sem, grads_sem, out_sem), comm = rest[:4], rest[4:]
    slots = comm[0]
    chips, (rows, d), ff = k * k, dy.shape, gate.shape[1]
    share = rows // RINGS
    core, a, b, positions = place(k)
    quarter = d // 4
    block = quarter // 4

    def given_copies(g):
        return [
            pltpu.make_async_copy(t.at[pl.ds(at, share)], given.at[g % 2, j, pl.ds(to, share)], given_sem.at[g % 2, j, i])
            for i, (to, at) in enumerate(token_rows(k, positions, g, share, rows)) for j, t in enumerate((gate, up))]

    def grads_copies(g):
        return [
            pltpu.make_async_copy(grads.at[g % 2, j, pl.ds(to, share)], t.at[pl.ds(at, share)], grads_sem.at[g % 2, j, i])
            for i, (to, at) in enumerate(token_rows(k, positions, g, share, rows)) for j, t in enumerate((dg, du))]

    w_copies = [pltpu.make_async_copy(w_down.at[:, pl.ds(i * quarter, quarter)], wd.at[i], w_sem.at[i]) for i in range(4)]
    for c in w_copies:
        c.start()
    for c in given_copies(0):
        c.start()

    @pl.loop(0, ff, step=64)
    def _(i):
        wacc[pl.ds(pl.multiple_of(i, 64), 64)] = jnp.zeros((64, d), F32)

    def before(g):
        @pl.when(g == 0)
        def _():
            for c in w_copies:
                c.wait()

        @pl.when(g + 1 < chips)
        def _():
            for c in given_copies(g + 1):
                c.start()

    def d_hidden(g):
        for i in range(4):
            term = lax.dot_general(slots[g % SLOTS, :, pl.ds(i * quarter, quarter)], wd[i], (((1,), (1,)), ((), ())), preferred_element_type=F32)
            hacc[...] = term if i == 0 else hacc[...] + term
        for c in given_copies(g):
            c.wait()

        @pl.when(g >= 2)
        def _():
            for c in grads_copies(g - 2):
                c.wait()

        @pl.loop(0, 2 * rows, step=2 * share)
        def _(i):
            at = pl.ds(pl.multiple_of(i, 2 * share), 2 * share)
            hidden, back = jax.vjp(act, given[g % 2, 0, at].astype(F32), given[g % 2, 1, at].astype(F32))
            for j, t in enumerate(back(hacc[at])):
                grads[g % 2, j, at] = t.astype(BF16)
            hid[at] = hidden.astype(BF16)
        for c in grads_copies(g):
            c.start()

    def d_down(g):
        @pl.loop(0, d, step=block)
        def _(i):
            at = pl.ds(pl.multiple_of(i, block), block)
            wacc[:, at] += lax.dot_general(hid[...], slots[g % SLOTS, :, at], (((0,), (0,)), ((), ())), preferred_element_type=F32)

    gather(k, 1, core, a, b, positions, dy, *comm, before, (d_hidden, d_down), lambda g: None)
    out_copies = []
    for j in range(ff // (2 * rows)):
        at = pl.ds(j * 2 * rows, 2 * rows)

        @pl.loop(0, d, step=block)
        def _(i):
            cols = pl.ds(pl.multiple_of(i, block), block)
            slots[j, :, cols] = wacc[at, cols].astype(BF16)
        out_copies.append(pltpu.make_async_copy(slots.at[j], dw.at[at], out_sem.at[j]))
        out_copies[-1].start()
    for c in out_copies + grads_copies(chips - 2) + grads_copies(chips - 1):
        c.wait()


def gather_hidden(k, dy, gate, up, w_down):
    (rows, d), (tokens, ff) = dy.shape, gate.shape
    dma = pltpu.SemaphoreType.DMA
    copies = (2, 2, 2 * RINGS)
    return pl.pallas_call(
        functools.partial(hidden_kernel, k),
        out_shape=[jax.ShapeDtypeStruct((tokens, ff), BF16)] * 2 + [jax.ShapeDtypeStruct((ff, d), BF16)],
        in_specs=[pl.BlockSpec(memory_space=pl.ANY)] * 4,
        out_specs=[pl.BlockSpec(memory_space=pl.ANY)] * 3,
        scratch_shapes=[
            pltpu.VMEM((4, ff, d // 4), BF16),
            pltpu.VMEM((ff, d), F32),
            pltpu.VMEM((2 * rows, ff), F32),
            pltpu.VMEM((2, 2, 2 * rows, ff), BF16),
            pltpu.VMEM((2 * rows, ff), BF16),
            pltpu.VMEM((2, 2, 2 * rows, ff), BF16),
            dma((4,)), dma(copies), dma(copies), dma((ff // (2 * rows),)),
            *gather_scratch(rows, d),
        ],
        compiler_params=pltpu.CompilerParams(collective_id=1, has_side_effects=True, vmem_limit_bytes=63 * 2**20),
        cost_estimate=pl.CostEstimate(flops=4 * tokens * ff * d, bytes_accessed=8 * tokens * ff, transcendentals=0),
        name="gather_hidden",
    )(dy, gate, up, w_down)


PASSES = 2
PIECES = 8


def weights_kernel(k, x, dg, du, dw_gate, dw_up, acc, grads, stage, *rest):
    (grads_sem, out_sem), comm = rest[:2], rest[2:]
    slots = comm[0]
    chips, rows, ff = k * k, x.shape[0], dg.shape[1]
    share, cols = rows // RINGS, slots.shape[2]
    core, a, b, positions = place(k)
    total = PASSES * chips
    high = cols // PIECES

    def grads_copies(g):
        return [
            pltpu.make_async_copy(t.at[pl.ds(at, share)], grads.at[g % 2, pl.ds(to, share), pl.ds(j * ff, ff)], grads_sem.at[g % 2, j, i])
            for i, (to, at) in enumerate(token_rows(k, positions, g, share, rows)) for j, t in enumerate((dg, du))]

    def out_copies(g, i):
        at = pl.ds(pl.multiple_of(g // chips * cols + i * high, high), high)
        return [pltpu.make_async_copy(stage.at[i, :, pl.ds(j * ff, ff)], t.at[at], out_sem.at[j, i]) for j, t in enumerate((dw_gate, dw_up))]

    for c in grads_copies(0):
        c.start()

    def before(g):
        @pl.when(g + 1 < total)
        def _():
            for c in grads_copies(g + 1):
                c.start()
        for c in grads_copies(g):
            c.wait()

    def piece(g, i):
        at = pl.ds(i * high, high)
        term = lax.dot_general(slots[g % SLOTS, :, at], grads[g % 2], (((0,), (0,)), ((), ())), preferred_element_type=F32)
        first, last = g % chips == 0, g % chips == chips - 1

        @pl.when(first)
        def _():
            acc[at] = term

        @pl.when(jnp.logical_not(first))
        def _():
            acc[at] += term

        @pl.when(last)
        def _():
            @pl.when(g >= chips)
            def _():
                for c in out_copies(g - chips, i):
                    c.wait()
            stage[i] = acc[at].astype(BF16)
            for c in out_copies(g, i):
                c.start()

    def some(h):
        def run(g):
            for i in range(h * PIECES // HALVES, (h + 1) * PIECES // HALVES):
                piece(g, i)
        return run

    gather(k, PASSES, core, a, b, positions, x, *comm, before, [some(h) for h in range(HALVES)], lambda g: None)
    for i in range(PIECES):
        for c in out_copies(total - 1, i):
            c.wait()


def gather_weights(k, x, dg, du):
    (rows, d), (tokens, ff) = x.shape, dg.shape
    cols = d // PASSES
    dma = pltpu.SemaphoreType.DMA
    return pl.pallas_call(
        functools.partial(weights_kernel, k),
        out_shape=[jax.ShapeDtypeStruct((d, ff), BF16)] * 2,
        in_specs=[pl.BlockSpec(memory_space=pl.ANY)] * 3,
        out_specs=[pl.BlockSpec(memory_space=pl.ANY)] * 2,
        scratch_shapes=[
            pltpu.VMEM((cols, 2 * ff), F32),
            pltpu.VMEM((2, 2 * rows, 2 * ff), BF16),
            pltpu.VMEM((PIECES, cols // PIECES, 2 * ff), BF16),
            dma((2, 2, 2 * RINGS)), dma((2, PIECES)),
            *gather_scratch(rows, cols),
        ],
        compiler_params=pltpu.CompilerParams(collective_id=2, has_side_effects=True, vmem_limit_bytes=63 * 2**20),
        cost_estimate=pl.CostEstimate(flops=4 * tokens * ff * d, bytes_accessed=8 * tokens * ff, transcendentals=0),
        name="gather_weights",
    )(x, dg, du)


def solution(mesh):
    k = math.isqrt(mesh.shape["tp"] // 2)

    def body(x, dy, gate, up, w_gate, w_up, w_down):
        d_gate, d_up, dw_down = gather_hidden(k, dy, gate, up, w_down)
        dw_gate, dw_up = gather_weights(k, x, d_gate, d_up)
        dx = scatter_dx(k, d_gate, d_up, w_gate, w_up)
        return dx, dw_gate, dw_up, dw_down

    rows, cols, grads = P(("dp", "tp"), None), P("dp", "tp"), P("dp", "tp")
    return jax.shard_map(
        body, mesh=mesh,
        in_specs=(rows, rows, cols, cols, P(None, "tp"), P(None, "tp"), P("tp", None)),
        out_specs=(rows, grads, grads, P(("dp", "tp"), None)), check_vma=False)
```

```python
import functools
import math

import jax
import jax.numpy as jnp
from jax import lax
from jax.experimental import pallas as pl
from jax.experimental.pallas import tpu as pltpu
from jax.sharding import PartitionSpec as P

F32, BF16 = jnp.float32, jnp.bfloat16
RINGS = 4
PARTS = 2
FETCH = 3
LEAD = 4


def act(gate, up):
    return jax.nn.silu(gate) * up


def place(k):
    me = lax.axis_index("tp")
    core, chip = me % 2, me // 2
    a, b = chip // k, chip % k
    s = (a + b) % k
    return core, a, b, (a * k + s, b * k + s)


def chip_at(k, cycle, position):
    a = position // k
    b = (position % k - a + k) % k
    return a * k + b if cycle == 0 else b * k + a


def on_ring(ring, position, steps, chips):
    return (position + steps + chips) % chips if ring % 2 == 0 else (position - steps + chips) % chips


def greet(k, core, a, b):
    chips = (((a + 1) % k) * k + b, ((a + k - 1) % k) * k + b, a * k + (b + 1) % k, a * k + (b + k - 1) % k)
    barrier = pltpu.get_barrier_semaphore()
    for chip in chips:
        pl.semaphore_signal(barrier, inc=1, device_id={"tp": chip * 2 + core})
    pl.semaphore_signal(barrier, inc=1, device_id={"tp": (a * k + b) * 2 + 1 - core})
    pl.semaphore_wait(barrier, 5)


def scatter_kernel(k, grads, wg, wu, out, wv, av, own, psend, precv, rsend, rrecv,
                   w_sem, a_sem, psend_sem, precv_sem, rsend_sem, rrecv_sem, out_sem):
    chips = k * k
    units, width, depth = wv.shape
    rows, ff = out.shape[0], depth // 2
    core, a, b, positions = place(k)
    partner = (a * k + b) * 2 + 1 - core
    order = [(r * PARTS + h, r, h) for h in range(PARTS) for r in range(RINGS)]

    def w_copies(u):
        cols = pl.ds(u * width, width)
        return [pltpu.make_async_copy(w.at[cols], wv.at[u, :, pl.ds(i * ff, ff)], w_sem.at[u, i]) for i, w in enumerate((wg, wu))]

    def a_copies(s, r):
        to = chip_at(k, r // 2, on_ring(r, positions[r // 2], -1 - s + chips, chips))
        copies = []
        for i, which in enumerate((core, 1 - core)):
            at = pl.ds((to * 2 + which) * rows, rows)
            copies.append(pltpu.make_async_copy(grads.at[at], av.at[s % 2, r, pl.ds(i * rows, rows)], a_sem.at[s % 2, r, i]))
        return copies

    def to_partner(s, u):
        return pltpu.make_async_remote_copy(
            psend.at[u], precv.at[s % 2, u], psend_sem.at[u], precv_sem.at[s % 2, u], device_id={"tp": partner})

    def to_next(s, u, r):
        to = chip_at(k, r // 2, on_ring(r, positions[r // 2], 1, chips)) * 2 + core
        return pltpu.make_async_remote_copy(
            rsend.at[s % 2, u], rrecv.at[(s + 1) % 3, u], rsend_sem.at[s % 2, u], rrecv_sem.at[(s + 1) % 3, u], device_id={"tp": to})

    def to_out(u):
        return pltpu.make_async_copy(rsend.at[(chips - 1) % 2, u], out.at[:, pl.ds(u * width, width)], out_sem.at[u])

    def multiply(s, u, r, h, first=False):
        if first:
            for c in w_copies(u):
                c.wait()
        if h == 0:
            for c in a_copies(s, r):
                c.wait()
        if not first:
            to_partner(s, u).wait_send()
        acc = lax.dot_general(av[s % 2, r], wv[u], (((1,), (1,)), ((), ())), preferred_element_type=F32)
        own[u] = acc[:rows]
        psend[u] = acc[rows:].astype(BF16)
        to_partner(s, u).start()

    def combine(s, u, r):
        to_partner(s, u).wait_recv()

        @pl.when(s >= 2)
        def _():
            to_next(s, u, r).wait_send()

        @pl.when(s == 0)
        def _():
            rsend[s % 2, u] = (own[u] + precv[s % 2, u].astype(F32)).astype(BF16)

        @pl.when(s > 0)
        def _():
            to_next(s - 1, u, r).wait_recv()
            rsend[s % 2, u] = (own[u] + precv[s % 2, u].astype(F32) + rrecv[s % 3, u].astype(F32)).astype(BF16)

        @pl.when(s < chips - 1)
        def _():
            to_next(s, u, r).start()

        @pl.when(s == chips - 1)
        def _():
            to_out(u).start()

    def fetch(i):
        if i < units:
            u, r, h = order[i]
            for c in (a_copies(0, r) if h == 0 else []) + w_copies(u):
                c.start()

    for i in range(FETCH):
        fetch(i)
    greet(k, core, a, b)
    for i, (u, r, h) in enumerate(order):
        fetch(i + FETCH)
        multiply(0, u, r, h, first=True)
        if i >= LEAD:
            combine(0, *order[i - LEAD][:2])
        if h == PARTS - 1:
            for c in a_copies(1, r):
                c.start()

    @pl.loop(0, chips)
    def _(s):
        @pl.when(s + 2 < chips)
        def _():
            for r in range(RINGS):
                for c in a_copies(s + 2, r):
                    c.start()
        for i, (u, r, h) in enumerate(order):
            late = units - LEAD + i

            @pl.when(s + 1 < chips)
            def _():
                multiply(s + 1, u, r, h)
            if late < units:
                combine(s, *order[late][:2])
            else:
                @pl.when(s + 1 < chips)
                def _():
                    combine(s + 1, *order[late - units][:2])

    for u, r, h in order:
        to_partner(chips - 1, u).wait_send()
        to_next(chips - 2, u, r).wait_send()
        to_out(u).wait()


def scatter_dx(k, grads, wg, wu):
    tokens, (d, ff) = grads.shape[0], wg.shape
    rows = tokens // (2 * k * k)
    units = RINGS * PARTS
    width = d // units
    dma = pltpu.SemaphoreType.DMA
    return pl.pallas_call(
        functools.partial(scatter_kernel, k),
        out_shape=jax.ShapeDtypeStruct((rows, d), BF16),
        in_specs=[pl.BlockSpec(memory_space=pl.ANY)] * 3,
        out_specs=pl.BlockSpec(memory_space=pl.ANY),
        scratch_shapes=[
            pltpu.VMEM((units, width, 2 * ff), BF16),
            pltpu.VMEM((2, RINGS, 2 * rows, 2 * ff), BF16),
            pltpu.VMEM((units, rows, width), F32),
            pltpu.VMEM((units, rows, width), BF16),
            pltpu.VMEM((2, units, rows, width), BF16),
            pltpu.VMEM((2, units, rows, width), BF16),
            pltpu.VMEM((3, units, rows, width), BF16),
            dma((units, 2)), dma((2, RINGS, 2)), dma((units,)), dma((2, units)), dma((2, units)), dma((3, units)), dma((units,)),
        ],
        compiler_params=pltpu.CompilerParams(collective_id=0, has_side_effects=True, vmem_limit_bytes=63 * 2**20),
        cost_estimate=pl.CostEstimate(flops=4 * tokens * ff * d, bytes_accessed=6 * tokens * ff + 4 * d * ff, transcendentals=0),
        name="scatter_dx",
    )(grads, wg, wu)


SLOTS = 4


def gather(k, passes, core, a, b, positions, src, slots, load_sem, next_sem, ring_sem, mate_send_sem, mate_sem, credit, before, pieces):
    chips = k * k
    total = passes * chips
    share, cols = slots.shape[1] // (2 * RINGS), slots.shape[2]
    width = cols // PARTS
    partner = (a * k + b) * 2 + 1 - core

    def part(g, r, h, which=core):
        at = pl.multiple_of((2 * r + which) * share, share)
        return slots.at[g % SLOTS, pl.ds(at, share), pl.ds(h * width, width)]

    def load(g, r, h):
        at = pl.multiple_of(g // chips * cols + h * width, width)
        return pltpu.make_async_copy(src.at[pl.ds(r * share, share), pl.ds(at, width)], part(g, r, h), load_sem.at[r, h])

    def to_next(g, r, h):
        to = chip_at(k, r // 2, on_ring(r, positions[r // 2], 1, chips)) * 2 + core
        return pltpu.make_async_remote_copy(
            part(g, r, h), part(g + 1, r, h), next_sem.at[g % SLOTS, r, h], ring_sem.at[(g + 1) % SLOTS, r, h], device_id={"tp": to})

    def to_mate(g, r, h):
        return pltpu.make_async_remote_copy(
            part(g, r, h), part(g, r, h), mate_send_sem.at[g % 2, r, h], mate_sem.at[g % SLOTS, r, h], device_id={"tp": partner})

    def came_from_mate(g, r, h):
        return pltpu.make_async_remote_copy(
            part(g, r, h), part(g, r, h, 1 - core), mate_send_sem.at[g % 2, r, h], mate_sem.at[g % SLOTS, r, h], device_id={"tp": partner})

    def pass_on(g, r, h):
        @pl.when(g == 0)
        def _():
            load(g, r, h).wait()

        @pl.when(g % chips > 0)
        def _():
            to_next(g - 1, r, h).wait_recv()

        early = jnp.where(g % chips == chips - 1, 1, 0)
        goes = jnp.where(g % chips == 0, jnp.where(g == 0, 1, 0), jnp.where(g + early < total, 1, 0))

        @pl.when(goes == 1)
        def _():
            @pl.when(early == 1)
            def _():
                load(g + 1, r, h).wait()
            if h == 0:
                @pl.when(g + early + 1 >= SLOTS)
                def _():
                    pl.semaphore_wait(credit.at[r], 1)
            to_next(g + early, r, h).start()

    both = [(r, h) for h in range(PARTS) for r in range(RINGS)]
    for r, h in both:
        load(0, r, h).start()
    greet(k, core, a, b)

    def pass_all(g, h):
        for r in range(RINGS):
            pass_on(g, r, h)
        for r in range(RINGS):
            to_mate(g, r, h).start()

    def compute(g, h):
        for r in range(RINGS):
            came_from_mate(g, r, h).wait_recv()
        pieces[h](g)

    @pl.loop(0, total + 1)
    def _(g):
        @pl.when(g == 0)
        def _():
            for h in range(PARTS):
                pass_all(g, h)
            before()

        for h in range(PARTS):
            @pl.when(jnp.logical_and(g > 0, g < total))
            def _():
                pass_all(g, h)

            @pl.when(g > 0 if h == 0 else g < total)
            def _():
                compute(g - 1 if h == 0 else g, (h - 1) % PARTS)

        @pl.when(g > 0)
        def _():
            for r, h in both:
                @pl.when((g - 1) % chips < chips - 1)
                def _():
                    to_next(g - 1, r, h).wait_send()
                to_mate(g - 1, r, h).wait_send()
            refill = g - 1 + SLOTS

            @pl.when(jnp.logical_and(refill < total, refill % chips > 0))
            def _():
                for r in range(RINGS):
                    frm = chip_at(k, r // 2, on_ring(r, positions[r // 2], -1, chips)) * 2 + core
                    pl.semaphore_signal(credit.at[r], inc=1, device_id={"tp": frm})

            @pl.when(jnp.logical_and(refill < total, refill % chips == 0))
            def _():
                for r, h in both:
                    load(refill, r, h).start()


def gather_scratch(rows, cols):
    dma, two = pltpu.SemaphoreType.DMA, (2, RINGS, PARTS)
    return [
        pltpu.VMEM((SLOTS, 2 * rows, cols), BF16),
        dma((RINGS, PARTS)), dma((SLOTS, RINGS, PARTS)), dma((SLOTS, RINGS, PARTS)), dma(two), dma((SLOTS, RINGS, PARTS)),
        pltpu.SemaphoreType.REGULAR((RINGS,)),
    ]


def token_rows(k, positions, g, share, rows):
    chips = k * k
    for r in range(RINGS):
        chip = chip_at(k, r // 2, on_ring(r, positions[r // 2], -(g % chips), chips))
        for c in range(2):
            yield (2 * r + c) * share, pl.multiple_of((chip * 2 + c) * rows + r * share, share)


def hidden_kernel(k, dy, gate, up, w_down, all_grads, dw, wd, wacc, hacc, given, hid, hid_t, grads, *rest):
    (w_sem, given_sem, grads_sem, out_sem), comm = rest[:4], rest[4:]
    slots = comm[0]
    chips, (rows, d), ff = k * k, dy.shape, gate.shape[1]
    share = rows // RINGS
    core, a, b, positions = place(k)
    quarter = d // PARTS
    block = d // 16

    def given_copies(g):
        return [
            pltpu.make_async_copy(t.at[pl.ds(at, share)], given.at[g % 2, j, pl.ds(to, share)], given_sem.at[g % 2, j, i])
            for i, (to, at) in enumerate(token_rows(k, positions, g, share, rows)) for j, t in enumerate((gate, up))]

    def grads_copies(g):
        return [
            pltpu.make_async_copy(grads.at[g % 2, pl.ds(to, share)], all_grads.at[pl.ds(at, share)], grads_sem.at[g % 2, i])
            for i, (to, at) in enumerate(token_rows(k, positions, g, share, rows))]

    w_copies = [pltpu.make_async_copy(w_down.at[:, pl.ds(i * quarter, quarter)], wd.at[i], w_sem.at[i]) for i in range(PARTS)]

    def before():
        for c in given_copies(0) + w_copies:
            c.start()

        @pl.loop(0, ff, step=64)
        def _(i):
            wacc[pl.ds(pl.multiple_of(i, 64), 64)] = jnp.zeros((64, d), F32)
        for c in w_copies:
            c.wait()

    def d_hidden(g, i):
        term = lax.dot_general(slots[g % SLOTS, :, pl.ds(i * quarter, quarter)], wd[i], (((1,), (1,)), ((), ())), preferred_element_type=F32)
        hacc[...] = term if i == 0 else hacc[...] + term

    def piece(i):
        def run(g):
            if i == 0:
                @pl.when(g + 1 < chips)
                def _():
                    for c in given_copies(g + 1):
                        c.start()
            d_hidden(g, i)
            if i == PARTS - 1:
                last(g)
        return run

    def last(g):
        for c in given_copies(g):
            c.wait()

        @pl.when(g >= 2)
        def _():
            for c in grads_copies(g - 2):
                c.wait()

        @pl.loop(0, 2 * rows, step=2 * share)
        def _(i):
            at = pl.ds(pl.multiple_of(i, 2 * share), 2 * share)
            hidden, back = jax.vjp(act, given[g % 2, 0, at].astype(F32), given[g % 2, 1, at].astype(F32))
            for j, t in enumerate(back(hacc[at])):
                grads[g % 2, at, pl.ds(j * ff, ff)] = t.astype(BF16)
            hid[at] = hidden.astype(BF16)
        for c in grads_copies(g):
            c.start()
        hid_t[...] = hid[...].T

        def term(at):
            return wacc[:, at] + jnp.dot(hid_t[...], slots[g % SLOTS, :, at], preferred_element_type=F32)

        @pl.when(g < chips - 1)
        def _():
            @pl.loop(0, d, step=block)
            def _(i):
                at = pl.ds(pl.multiple_of(i, block), block)
                wacc[:, at] = term(at)

        @pl.when(g == chips - 1)
        def _():
            @pl.loop(0, d // block)
            def _(i):
                at = pl.ds(pl.multiple_of(i * block, block), block)
                done = term(at).astype(BF16)
                for j in range(ff // (2 * rows)):
                    slots[j, :, at] = done[2 * rows * j:2 * rows * (j + 1)]
                    out_copy(i, j).start()

    def out_copy(i, j):
        at = pl.ds(pl.multiple_of(i * block, block), block)
        return pltpu.make_async_copy(slots.at[j, :, at], dw.at[pl.ds(2 * rows * j, 2 * rows), at], out_sem.at[i, j])

    gather(k, 1, core, a, b, positions, dy, *comm, before, [piece(i) for i in range(PARTS)])

    @pl.loop(0, d // block)
    def _(i):
        for j in range(ff // (2 * rows)):
            out_copy(i, j).wait()
    for c in grads_copies(chips - 2) + grads_copies(chips - 1):
        c.wait()


def gather_hidden(k, dy, gate, up, w_down):
    (rows, d), (tokens, ff) = dy.shape, gate.shape
    dma = pltpu.SemaphoreType.DMA
    copies = (2, 2, 2 * RINGS)
    return pl.pallas_call(
        functools.partial(hidden_kernel, k),
        out_shape=[jax.ShapeDtypeStruct((tokens, 2 * ff), BF16), jax.ShapeDtypeStruct((ff, d), BF16)],
        in_specs=[pl.BlockSpec(memory_space=pl.ANY)] * 4,
        out_specs=[pl.BlockSpec(memory_space=pl.ANY)] * 2,
        scratch_shapes=[
            pltpu.VMEM((PARTS, ff, d // PARTS), BF16),
            pltpu.VMEM((ff, d), F32),
            pltpu.VMEM((2 * rows, ff), F32),
            pltpu.VMEM((2, 2, 2 * rows, ff), BF16),
            pltpu.VMEM((2 * rows, ff), BF16),
            pltpu.VMEM((ff, 2 * rows), BF16),
            pltpu.VMEM((2, 2 * rows, 2 * ff), BF16),
            dma((PARTS,)), dma(copies), dma((2, 2 * RINGS)), dma((16, ff // (2 * rows))),
            *gather_scratch(rows, d),
        ],
        compiler_params=pltpu.CompilerParams(collective_id=1, has_side_effects=True, vmem_limit_bytes=63 * 2**20),
        cost_estimate=pl.CostEstimate(flops=4 * tokens * ff * d, bytes_accessed=8 * tokens * ff, transcendentals=0),
        name="gather_hidden",
    )(dy, gate, up, w_down)


PASSES = 2
PIECES = 8


def weights_kernel(k, x, all_grads, dw_gate, dw_up, acc, grads, stage, *rest):
    (grads_sem, out_sem), comm = rest[:2], rest[2:]
    slots = comm[0]
    chips, rows, ff = k * k, x.shape[0], dw_gate.shape[1]
    share, cols = rows // RINGS, slots.shape[2]
    core, a, b, positions = place(k)
    total = PASSES * chips
    high = cols // PIECES

    def grads_copies(g):
        return [
            pltpu.make_async_copy(all_grads.at[pl.ds(at, share)], grads.at[g % 2, pl.ds(to, share)], grads_sem.at[g % 2, i])
            for i, (to, at) in enumerate(token_rows(k, positions, g, share, rows))]

    def out_copies(g, i):
        at = pl.ds(pl.multiple_of(g // chips * cols + i * high, high), high)
        return [pltpu.make_async_copy(stage.at[i, :, pl.ds(j * ff, ff)], t.at[at], out_sem.at[j, i]) for j, t in enumerate((dw_gate, dw_up))]

    def before():
        for c in grads_copies(0):
            c.start()

        @pl.loop(0, cols, step=high)
        def _(i):
            acc[pl.ds(pl.multiple_of(i, high), high)] = jnp.zeros((high, 2 * ff), F32)

    def piece(g, i):
        at = pl.ds(i * high, high)
        acc[at] += lax.dot_general(slots[g % SLOTS, :, at], grads[g % 2], (((0,), (0,)), ((), ())), preferred_element_type=F32)

        @pl.when(g % chips == chips - 1)
        def _():
            @pl.when(g >= chips)
            def _():
                for c in out_copies(g - chips, i):
                    c.wait()
            stage[i] = acc[at].astype(BF16)
            acc[at] = jnp.zeros((high, 2 * ff), F32)
            for c in out_copies(g, i):
                c.start()

    def some(h):
        def run(g):
            if h == 0:
                @pl.when(g + 1 < total)
                def _():
                    for c in grads_copies(g + 1):
                        c.start()
                for c in grads_copies(g):
                    c.wait()
            for i in range(h * PIECES // PARTS, (h + 1) * PIECES // PARTS):
                piece(g, i)
        return run

    gather(k, PASSES, core, a, b, positions, x, *comm, before, [some(h) for h in range(PARTS)])
    for i in range(PIECES):
        for c in out_copies(total - 1, i):
            c.wait()


def gather_weights(k, x, grads):
    (rows, d), (tokens, ff) = x.shape, (grads.shape[0], grads.shape[1] // 2)
    cols = d // PASSES
    dma = pltpu.SemaphoreType.DMA
    return pl.pallas_call(
        functools.partial(weights_kernel, k),
        out_shape=[jax.ShapeDtypeStruct((d, ff), BF16)] * 2,
        in_specs=[pl.BlockSpec(memory_space=pl.ANY)] * 2,
        out_specs=[pl.BlockSpec(memory_space=pl.ANY)] * 2,
        scratch_shapes=[
            pltpu.VMEM((cols, 2 * ff), F32),
            pltpu.VMEM((2, 2 * rows, 2 * ff), BF16),
            pltpu.VMEM((PIECES, cols // PIECES, 2 * ff), BF16),
            dma((2, 2 * RINGS)), dma((2, PIECES)),
            *gather_scratch(rows, cols),
        ],
        compiler_params=pltpu.CompilerParams(collective_id=2, has_side_effects=True, vmem_limit_bytes=63 * 2**20),
        cost_estimate=pl.CostEstimate(flops=4 * tokens * ff * d, bytes_accessed=8 * tokens * ff, transcendentals=0),
        name="gather_weights",
    )(x, grads)


def hand_over_kernel(*refs):
    count = len(refs) // 3
    arrays, (load_sem, store_sem) = list(zip(refs[:count], refs[count:2 * count], refs[2 * count:3 * count])), refs[3 * count:]
    moves = []
    for i, (src, dst, mid) in enumerate(arrays):
        high = src.shape[0] // PIECES
        for j in range(PIECES):
            at = pl.ds(j * high, high)
            moves.append((pltpu.make_async_copy(src.at[at], mid.at[at], load_sem.at[i, j]),
                          pltpu.make_async_copy(mid.at[at], dst.at[at], store_sem.at[i, j])))
    for load, _ in moves:
        load.start()
    for load, store in moves:
        load.wait()
        store.start()
    for _, store in moves:
        store.wait()


def hand_over(*arrays):
    dma = pltpu.SemaphoreType.DMA((len(arrays), PIECES))
    return pl.pallas_call(
        hand_over_kernel,
        out_shape=[jax.ShapeDtypeStruct(t.shape, t.dtype) for t in arrays],
        in_specs=[pl.BlockSpec(memory_space=pl.ANY)] * len(arrays),
        out_specs=[pl.BlockSpec(memory_space=pl.ANY)] * len(arrays),
        scratch_shapes=[*(pltpu.VMEM(t.shape, t.dtype) for t in arrays), dma, dma],
        compiler_params=pltpu.CompilerParams(vmem_limit_bytes=63 * 2**20),
        name="hand_over",
    )(*arrays)


def solution(mesh):
    k = math.isqrt(mesh.shape["tp"] // 2)

    def body(x, dy, gate, up, w_gate, w_up, w_down):
        grads, dw_down = gather_hidden(k, dy, gate, up, w_down)
        dw_gate, dw_up = gather_weights(k, x, grads)
        dx = scatter_dx(k, grads, w_gate, w_up)
        return tuple(hand_over(dx, dw_gate, dw_up, dw_down))

    rows, cols, sums = P(("dp", "tp"), None), P("dp", "tp"), P("dp", "tp")
    return jax.shard_map(
        body, mesh=mesh,
        in_specs=(rows, rows, cols, cols, P(None, "tp"), P(None, "tp"), P("tp", None)),
        out_specs=(rows, sums, sums, P(("dp", "tp"), None)), check_vma=False)
```
